512 devices in a mesh: sub: 64 (over x, y_lo, z), agg: 8 (over y_hi, core).
Axes of the slice: x: 4, y: 8 (y_hi: 4, y_lo: 2; y = y_hi * 2 + y_lo), z: 8, core: 2. Of those that a mesh axis runs over, the one named last changes fastest.
Arguments:
- block_values: float32 [7, 4, 4, 524288], P(None, None, None, ('sub', 'agg'))
- block_cols: int32 [7, 524288], P(None, ('sub', 'agg')), may hold values from 0 to 524287, as said below
- coarse_rhs: float32 [4, 524288], P(None, ('sub', 'agg'))
- guess: float32 [4, 524288], P(None, ('sub', 'agg')), may hold values from -3 to 3
- bound_low: int32 [1], replicated, may hold values from 20 to 26
- bound_high: int32 [1], replicated, may hold values from 32 to 40
Outputs:
- smoothed: float32 [4, 524288], P(None, ('sub', 'agg'))
- residual: float32 [4, 524288], P(None, ('sub', 'agg'))
- residual_rms: float32 [1], replicated
The draws below stay inside these ranges and needn't reach their ends.
Inputs may be any that keep to these rules, and one draw needn't show every extreme that they name: Block rows form 524288 / 1024 planes of 1024 consecutive rows, in a periodic order. block_cols[0] is the row itself, block_cols[1] a row of the previous plane, block_cols[2] a row of the next plane, block_cols[3] to block_cols[6] rows of the same plane.
All inputs are finite; a program needn't handle non-finite values.
Results may differ from the reference program's by a relative error of at most 0.0001.
Values sent between devices are 32-bit elements; how exact they have to be, the bound alone decides.
A program may use at most 64 MiB of HBM per device.

```python
import jax
import jax.numpy as jnp
from jax import lax

ROWS_DEV = 1024
COMP = 4
NEIGHBORS = 7
STEPS = 4
TOTAL = 524288


def draw_block_values(key, part):
    noise = 0.5 * jax.random.normal(key, (NEIGHBORS, COMP, COMP, TOTAL), jnp.float32)
    identity = jnp.eye(COMP, dtype=jnp.float32)[:, :, None]
    diagonal_block = noise[0] * (1.0 - identity) + 6.0 * identity
    return jnp.concatenate([diagonal_block[None], noise[1:]], axis=0)


def draw_block_cols(key, part):
    planes = TOTAL // ROWS_DEV
    rows_all = jnp.arange(TOTAL, dtype=jnp.int32)
    plane_of = rows_all // ROWS_DEV
    picked = jax.random.randint(key, (6, TOTAL), 0, ROWS_DEV).astype(jnp.int32)
    before = (plane_of - 1) % planes * ROWS_DEV + picked[0]
    after = (plane_of + 1) % planes * ROWS_DEV + picked[1]
    same_plane = plane_of[None, :] * ROWS_DEV + picked[2:]
    return jnp.concatenate([rows_all[None], before[None], after[None], same_plane], axis=0).astype(jnp.int32)


def draw_coarse_rhs(key, part):
    rows_all = jnp.arange(TOTAL, dtype=jnp.float32)
    scale_row = 0.5 + 0.5 * rows_all / TOTAL
    values = jax.random.normal(key, (COMP, TOTAL), jnp.float32)
    return values * scale_row[None, :]


def steps_of(own_key, extent, cuts, least, high):
    loudness = 1.0
    for dim, shards_of in cuts:
        draws = jax.random.uniform(jax.random.fold_in(jax.random.fold_in(own_key, 6), dim), (shards_of,), jnp.float32, least / len(cuts), high / len(cuts))
        loudness = loudness * jnp.repeat(jnp.exp(draws), extent[dim] // shards_of).reshape((-1,) + (1,) * (len(extent) - 1 - dim))
    return loudness


def scatter_about(rng, shape, scale, limit, cuts=(), held_as=jnp.bfloat16):
    array = jax.random.normal(rng, shape, jnp.float32) * scale
    if len(cuts) > 0:
        array = steps_of(rng, shape, cuts, -0.22, 0.18) * array
    return jnp.clip(array, min=-limit, max=limit).astype(held_as)


def setup_inputs(seed: int = 0) -> dict:
    splits = jax.random.split(jax.random.key(seed), 7)
    block_values = draw_block_values(jax.random.fold_in(splits[6], 71), 0)
    block_cols = draw_block_cols(jax.random.fold_in(splits[6], 71), 0)
    coarse_rhs = draw_coarse_rhs(jax.random.fold_in(splits[6], 71), 0)
    guess = scatter_about(splits[3], (COMP, TOTAL), 0.5, 3.0, ((1, 512),), jnp.float32)
    bound_low = jax.random.randint(splits[4], (1,), 20, 27).astype(jnp.int32)
    bound_high = jax.random.randint(splits[5], (1,), 32, 41).astype(jnp.int32)
    return dict(block_values=block_values, block_cols=block_cols, coarse_rhs=coarse_rhs, guess=guess, bound_low=bound_low, bound_high=bound_high)


def apply_blocks(block_values, position, field):
    count = position.shape[0]
    width = position.shape[1]
    taken = jnp.take(field, position.reshape(-1), axis=1).reshape(field.shape[0], count, width)
    result = jnp.zeros((field.shape[0], width), jnp.float32)
    for column in range(field.shape[0]):
        result = result + lax.optimization_barrier(jnp.sum(block_values[:, :, column, :] * taken[column][:, None, :], axis=0))
    return result

def reference(block_values, block_cols, coarse_rhs, guess, bound_low, bound_high):
    lower = bound_low[0].astype(jnp.float32) / 4.0
    upper = bound_high[0].astype(jnp.float32) / 4.0
    centre = (upper + lower) / 2.0
    half_width = (upper - lower) / 2.0
    spread_ratio = centre / half_width
    ratio_prev = 1.0 / spread_ratio
    smoothed = guess
    residual = coarse_rhs - apply_blocks(block_values, block_cols, guess)
    direction = residual / centre
    for step in range(STEPS):
        smoothed = smoothed + direction
        residual = residual - apply_blocks(block_values, block_cols, direction)
        if step + 1 < STEPS:
            ratio_next = 1.0 / (2.0 * spread_ratio - ratio_prev)
            direction = ratio_next * ratio_prev * direction + 2.0 * ratio_next / half_width * residual
            ratio_prev = ratio_next
    total_sq = jnp.sum(residual * residual)
    residual_rms = jnp.sqrt(total_sq / (4.0 * TOTAL) + 1e-06).reshape(1)
    return (smoothed, residual, residual_rms)
```

```python
import jax
import jax.numpy as jnp
from jax import lax
from jax.experimental import pallas as pl
from jax.experimental.pallas import tpu as pltpu
from jax.sharding import Mesh
from jax.sharding import PartitionSpec as P

STEPS = 4
COMP = 4
BLOCKS = 7
AXES = ("x", "yl", "z", "yh", "c")
SIZES = (4, 2, 8, 4, 2)
MESH_ID = pl.DeviceIdType.MESH


def plane_device(plane):
    coords = []
    for size in reversed(SIZES):
        coords.append(lax.rem(plane, size))
        plane = lax.div(plane, size)
    return tuple(reversed(coords))


def own_plane():
    plane = lax.axis_index(AXES[0])
    for name, size in zip(AXES[1:], SIZES[1:]):
        plane = plane * size + lax.axis_index(name)
    return plane


def smoother(values_hbm, cols_hbm, rhs_hbm, guess_hbm, low_hbm, high_hbm,
             smoothed_hbm, residual_hbm, square_hbm,
             values, cols, packed, low, high, sent, below, above, shown, square,
             load_sem, store_sem, below_send, below_recv, above_send, above_recv):
    planes = 1
    for size in SIZES:
        planes *= size
    me = own_plane()
    prev_dev = plane_device(lax.rem(me + planes - 1, planes))
    next_dev = plane_device(lax.rem(me + 1, planes))

    barrier = pltpu.get_barrier_semaphore()
    pl.semaphore_signal(barrier, inc=1, device_id=prev_dev, device_id_type=MESH_ID)
    pl.semaphore_signal(barrier, inc=1, device_id=next_dev, device_id_type=MESH_ID)

    loads = [
        pltpu.make_async_copy(guess_hbm, packed.at[0], load_sem.at[0]),
        pltpu.make_async_copy(low_hbm, low, load_sem.at[1]),
        pltpu.make_async_copy(high_hbm, high, load_sem.at[2]),
        pltpu.make_async_copy(cols_hbm, cols, load_sem.at[3]),
        pltpu.make_async_copy(rhs_hbm, packed.at[1], load_sem.at[4]),
        pltpu.make_async_copy(values_hbm, values, load_sem.at[5]),
    ]
    for load in loads:
        load.start()

    def unpack(ref):
        return [ref[pl.ds(c, 8, stride=COMP), :] for c in range(COMP)]

    def exchange(slot):
        copies = [
            pltpu.make_async_remote_copy(
                sent.at[slot], below.at[slot], below_send.at[slot], below_recv.at[slot],
                device_id=next_dev, device_id_type=MESH_ID),
            pltpu.make_async_remote_copy(
                sent.at[slot], above.at[slot], above_send.at[slot], above_recv.at[slot],
                device_id=prev_dev, device_id_type=MESH_ID),
        ]
        for copy in copies:
            copy.start()
        return copies

    loads[0].wait()
    field = unpack(packed.at[0])
    for c in range(COMP):
        sent[0, c] = field[c]
    pl.semaphore_wait(barrier, 2)
    copies = exchange(0)

    loads[1].wait()
    loads[2].wait()
    lower = jnp.full((8, 128), low[0], jnp.int32).astype(jnp.float32) / 4.0
    upper = jnp.full((8, 128), high[0], jnp.int32).astype(jnp.float32) / 4.0
    centre = (upper + lower) / 2.0
    half_width = (upper - lower) / 2.0
    spread_ratio = centre / half_width
    ratio = 1.0 / spread_ratio

    loads[3].wait()
    lanes, masks = {}, {}
    for k in range(1, BLOCKS):
        index = jnp.concatenate([cols[k:k + 1, t * 128:(t + 1) * 128] for t in range(8)], axis=0)
        lanes[k] = index & 127
        masks[k] = [(index & (128 << b)) != 0 for b in range(3)]

    def taken(ref, c, k):
        parts = []
        for t in range(8):
            chunk = jnp.broadcast_to(ref[c, t:t + 1, :], (8, 128))
            parts.append(jnp.take_along_axis(chunk, lanes[k], axis=1, mode="promise_in_bounds"))
        for b in range(3):
            parts = [jnp.where(masks[k][b], parts[2 * i + 1], parts[2 * i]) for i in range(len(parts) // 2)]
        return parts[0]

    def add_block(total, k, column, gathered):
        for i in range(COMP):
            block = values[k, i, pl.ds(column, 8, stride=COMP), :]
            total[i] = total[i] - block * gathered

    def subtract_own(residual, field, slot):
        total = list(residual)
        for j in range(COMP):
            add_block(total, 0, j, field[j])
        for k in range(3, BLOCKS):
            for j in range(COMP):
                add_block(total, k, j, taken(sent.at[slot], j, k))
        return total

    def subtract_far(total, slot):
        total = list(total)
        for k, ref in ((1, below), (2, above)):
            for j in range(COMP):
                add_block(total, k, j, taken(ref.at[slot], j, k))
        return total

    loads[4].wait()
    loads[5].wait()
    smoothed = field
    residual = unpack(packed.at[1])
    pending = []
    direction = field
    for slot in range(STEPS + 1):
        residual = subtract_own(residual, direction, slot)
        for copy in copies:
            copy.wait_recv()
        pending += copies
        residual = subtract_far(residual, slot)
        if slot == 0:
            direction = [r / centre for r in residual]
        elif slot < STEPS:
            following = 1.0 / (2.0 * spread_ratio - ratio)
            keep = following * ratio
            gain = 2.0 * following / half_width
            direction = [keep * d + gain * r for d, r in zip(direction, residual)]
            ratio = following
        if slot < STEPS:
            for c in range(COMP):
                sent[slot + 1, c] = direction[c]
            copies = exchange(slot + 1)
            smoothed = [s + d for s, d in zip(smoothed, direction)]
    for c in range(COMP):
        shown[0, pl.ds(c, 8, stride=COMP), :] = smoothed[c]
        shown[1, pl.ds(c, 8, stride=COMP), :] = residual[c]
    square[...] = sum(r * r for r in residual)
    stores = [
        pltpu.make_async_copy(shown.at[0], smoothed_hbm, store_sem.at[0]),
        pltpu.make_async_copy(shown.at[1], residual_hbm, store_sem.at[1]),
        pltpu.make_async_copy(square, square_hbm, store_sem.at[2]),
    ]
    for store in stores:
        store.start()
    for copy in pending:
        copy.wait_send()
    for store in stores:
        store.wait()


def shards(block_values, block_cols, coarse_rhs, guess, bound_low, bound_high):
    rows = block_values.shape[3]

    def packed_rows(a):
        lead = a.shape[:-2]
        a = a.reshape(*lead, COMP, rows // 128, 128)
        return jnp.swapaxes(a, -3, -2).reshape(*lead, COMP * rows // 128, 128)

    def unpacked_rows(a):
        return jnp.swapaxes(a.reshape(rows // 128, COMP, 128), 0, 1).reshape(COMP, rows)

    def hbm():
        return pl.BlockSpec(memory_space=pl.ANY)

    slots = STEPS + 1
    field = jax.ShapeDtypeStruct((32, 128), jnp.float32)
    smoothed, residual, square = pl.pallas_call(
        smoother,
        out_shape=(field, field, jax.ShapeDtypeStruct((8, 128), jnp.float32)),
        in_specs=[hbm()] * 6,
        out_specs=(hbm(),) * 3,
        scratch_shapes=[
            pltpu.VMEM((BLOCKS, COMP, 32, 128), jnp.float32),
            pltpu.VMEM((BLOCKS, rows), jnp.int32),
            pltpu.VMEM((2, 32, 128), jnp.float32),
            pltpu.SMEM((1,), jnp.int32),
            pltpu.SMEM((1,), jnp.int32),
            pltpu.VMEM((slots, COMP, 8, 128), jnp.float32),
            pltpu.VMEM((slots, COMP, 8, 128), jnp.float32),
            pltpu.VMEM((slots, COMP, 8, 128), jnp.float32),
            pltpu.VMEM((2, 32, 128), jnp.float32),
            pltpu.VMEM((8, 128), jnp.float32),
            pltpu.SemaphoreType.DMA((6,)),
            pltpu.SemaphoreType.DMA((3,)),
            pltpu.SemaphoreType.DMA((slots,)),
            pltpu.SemaphoreType.DMA((slots,)),
            pltpu.SemaphoreType.DMA((slots,)),
            pltpu.SemaphoreType.DMA((slots,)),
        ],
        compiler_params=pltpu.CompilerParams(collective_id=0, has_side_effects=True),
        name="smoother",
    )(packed_rows(block_values), block_cols, packed_rows(coarse_rhs), packed_rows(guess), bound_low, bound_high)
    total_sq = lax.psum(jnp.sum(square), AXES)
    count = COMP * rows * lax.axis_size(AXES)
    rms = jnp.sqrt(total_sq / (1.0 * count) + 1e-06).reshape(1)
    return unpacked_rows(smoothed), unpacked_rows(residual), rms


def solution(mesh):
    finer = Mesh(mesh.devices.reshape(SIZES), AXES)
    return jax.shard_map(
        shards,
        mesh=finer,
        in_specs=(
            P(None, None, None, AXES),
            P(None, AXES),
            P(None, AXES),
            P(None, AXES),
            P(),
            P(),
        ),
        out_specs=(P(None, AXES), P(None, AXES), P()),
        check_vma=False,
    )
```

```python
import jax
import jax.numpy as jnp
from jax import lax
from jax.experimental import pallas as pl
from jax.experimental.pallas import tpu as pltpu
from jax.sharding import Mesh
from jax.sharding import PartitionSpec as P

STEPS = 4
COMP = 4
BLOCKS = 7
AXES = ("x", "yl", "z", "yh", "c")
SIZES = (4, 2, 8, 4, 2)
MESH_ID = pl.DeviceIdType.MESH


def plane_device(plane):
    coords = []
    for size in reversed(SIZES):
        coords.append(lax.rem(plane, size))
        plane = lax.div(plane, size)
    return tuple(reversed(coords))


def own_plane():
    plane = lax.axis_index(AXES[0])
    for name, size in zip(AXES[1:], SIZES[1:]):
        plane = plane * size + lax.axis_index(name)
    return plane


def smoother(values_hbm, cols_hbm, rhs_hbm, guess_hbm, low_hbm, high_hbm,
             smoothed_hbm, residual_hbm, rms_out,
             values, cols, packed, low, high, sent, below, above, shown, partial, line, sheet,
             load_sem, store_sem, below_send, below_recv, above_send, above_recv,
             line_send, line_recv, sheet_send, sheet_recv, ready):
    planes = 1
    for size in SIZES:
        planes *= size
    me = own_plane()
    prev_dev = plane_device(lax.rem(me + planes - 1, planes))
    next_dev = plane_device(lax.rem(me + 1, planes))

    x, yl, z, yh, core = (lax.axis_index(name) for name in AXES)
    y = yh * 2 + yl

    def on_line(step):
        other = lax.rem(z * 2 + core + step, 16)
        return x, yl, lax.div(other, 2), yh, lax.rem(other, 2)

    def on_sheet(step):
        other = lax.rem(x * 8 + y + step, 32)
        other_y = lax.rem(other, 8)
        return lax.div(other, 8), lax.rem(other_y, 2), z, lax.div(other_y, 2), core

    def on_row(step):
        other_y = lax.rem(y + step, 8)
        return x, lax.rem(other_y, 2), z, lax.div(other_y, 2), core

    def on_column(step):
        return lax.rem(x + step, 4), yl, z, yh, core

    greeted = [prev_dev, next_dev]
    greeted += [on_line(step) for step in range(1, 16)]
    greeted += [on_row(step) for step in range(1, 8)]
    greeted += [on_column(step) for step in range(1, 4)]
    barrier = pltpu.get_barrier_semaphore()
    for device in greeted:
        pl.semaphore_signal(barrier, inc=1, device_id=device, device_id_type=MESH_ID)

    loads = [
        pltpu.make_async_copy(guess_hbm, packed.at[0], load_sem.at[0]),
        pltpu.make_async_copy(low_hbm, low, load_sem.at[1]),
        pltpu.make_async_copy(high_hbm, high, load_sem.at[2]),
        pltpu.make_async_copy(cols_hbm, cols, load_sem.at[3]),
        pltpu.make_async_copy(rhs_hbm, packed.at[1], load_sem.at[4]),
        pltpu.make_async_copy(values_hbm, values, load_sem.at[5]),
    ]
    for load in loads:
        load.start()

    def unpack(ref):
        return [ref[pl.ds(c, 8, stride=COMP), :] for c in range(COMP)]

    def exchange(slot):
        copies = [
            pltpu.make_async_remote_copy(
                sent.at[slot], below.at[slot], below_send.at[slot], below_recv.at[slot],
                device_id=next_dev, device_id_type=MESH_ID),
            pltpu.make_async_remote_copy(
                sent.at[slot], above.at[slot], above_send.at[slot], above_recv.at[slot],
                device_id=prev_dev, device_id_type=MESH_ID),
        ]
        for copy in copies:
            copy.start()
        return copies

    loads[0].wait()
    field = unpack(packed.at[0])
    for c in range(COMP):
        sent[0, c] = field[c]
    pl.semaphore_wait(barrier, len(greeted))
    copies = exchange(0)
    for step in range(1, 8):
        pl.semaphore_signal(ready, inc=1, device_id=on_row(step), device_id_type=MESH_ID)

    loads[1].wait()
    loads[2].wait()
    lower = jnp.full((8, 128), low[0], jnp.int32).astype(jnp.float32) / 4.0
    upper = jnp.full((8, 128), high[0], jnp.int32).astype(jnp.float32) / 4.0
    centre = (upper + lower) / 2.0
    half_width = (upper - lower) / 2.0
    spread_ratio = centre / half_width
    ratio = 1.0 / spread_ratio

    loads[3].wait()
    lanes, masks = {}, {}
    for k in range(1, BLOCKS):
        index = jnp.concatenate([cols[k:k + 1, t * 128:(t + 1) * 128] for t in range(8)], axis=0)
        lanes[k] = index & 127
        masks[k] = [(index & (128 << b)) != 0 for b in range(3)]

    def taken(ref, c, k):
        parts = []
        for t in range(8):
            chunk = jnp.broadcast_to(ref[c, t:t + 1, :], (8, 128))
            parts.append(jnp.take_along_axis(chunk, lanes[k], axis=1, mode="promise_in_bounds"))
        for b in range(3):
            parts = [jnp.where(masks[k][b], parts[2 * i + 1], parts[2 * i]) for i in range(len(parts) // 2)]
        return parts[0]

    def add_block(total, k, column, gathered):
        for i in range(COMP):
            block = values[k, i, pl.ds(column, 8, stride=COMP), :]
            total[i] = total[i] - block * gathered

    def subtract_own(residual, field, slot):
        total = list(residual)
        for j in range(COMP):
            add_block(total, 0, j, field[j])
        for k in range(3, BLOCKS):
            for j in range(COMP):
                add_block(total, k, j, taken(sent.at[slot], j, k))
        return total

    def subtract_far(total, slot):
        total = list(total)
        for k, ref in ((1, below), (2, above)):
            for j in range(COMP):
                add_block(total, k, j, taken(ref.at[slot], j, k))
        return total

    loads[4].wait()
    loads[5].wait()
    smoothed = field
    residual = unpack(packed.at[1])
    pending = []
    direction = field
    for slot in range(STEPS + 1):
        residual = subtract_own(residual, direction, slot)
        for copy in copies:
            copy.wait_recv()
        pending += copies
        residual = subtract_far(residual, slot)
        if slot == 0:
            direction = [r / centre for r in residual]
        elif slot < STEPS:
            following = 1.0 / (2.0 * spread_ratio - ratio)
            keep = following * ratio
            gain = 2.0 * following / half_width
            direction = [keep * d + gain * r for d, r in zip(direction, residual)]
            ratio = following
        if slot < STEPS:
            for c in range(COMP):
                sent[slot + 1, c] = direction[c]
            copies = exchange(slot + 1)
            smoothed = [s + d for s, d in zip(smoothed, direction)]
    for c in range(COMP):
        shown[0, pl.ds(c, 8, stride=COMP), :] = smoothed[c]
        shown[1, pl.ds(c, 8, stride=COMP), :] = residual[c]
    stores = [
        pltpu.make_async_copy(shown.at[0], smoothed_hbm, store_sem.at[0]),
        pltpu.make_async_copy(shown.at[1], residual_hbm, store_sem.at[1]),
    ]
    squares = jnp.sum(sum(r * r for r in residual), axis=0, keepdims=True)

    def spread(value, slots, own, device, peers, send_sem, recv_sem):
        partial[...] = value
        slots[own] = value
        sends = []
        for step in range(1, peers):
            send = pltpu.make_async_remote_copy(
                partial, slots.at[own], send_sem, recv_sem,
                device_id=device(step), device_id_type=MESH_ID)
            send.start()
            sends.append(send)
        arrived = slots.at[pl.ds(0, peers - 1)]
        pltpu.make_async_copy(arrived, arrived, recv_sem).wait()
        total = slots[0]
        for peer in range(1, peers):
            total = total + slots[peer]
        pltpu.make_async_copy(arrived, arrived, send_sem).wait()
        return total

    squares = spread(squares, line, z * 2 + core, on_line, 16, line_send, line_recv)
    for store in stores:
        store.start()
    pl.semaphore_wait(ready, 7)
    squares = spread(squares, sheet, x * 8 + y, on_sheet, 32, sheet_send, sheet_recv)
    total = jnp.sum(squares, axis=1, keepdims=True)
    entries = planes * COMP * 8 * 128
    rms = jnp.sqrt(total / (1.0 * entries) + 1e-06)
    rms_out[0] = rms[0, 0]
    for copy in pending:
        copy.wait_send()
    for store in stores:
        store.wait()


def shards(block_values, block_cols, coarse_rhs, guess, bound_low, bound_high):
    rows = block_values.shape[3]

    def packed_rows(a):
        lead = a.shape[:-2]
        a = a.reshape(*lead, COMP, rows // 128, 128)
        return jnp.swapaxes(a, -3, -2).reshape(*lead, COMP * rows // 128, 128)

    def unpacked_rows(a):
        return jnp.swapaxes(a.reshape(rows // 128, COMP, 128), 0, 1).reshape(COMP, rows)

    def hbm():
        return pl.BlockSpec(memory_space=pltpu.HBM)

    slots = STEPS + 1
    field = jax.ShapeDtypeStruct((32, 128), jnp.float32)
    smoothed, residual, rms = pl.pallas_call(
        smoother,
        out_shape=(field, field, jax.ShapeDtypeStruct((1,), jnp.float32)),
        in_specs=[hbm()] * 6,
        out_specs=(hbm(), hbm(), pl.BlockSpec(memory_space=pltpu.SMEM)),
        scratch_shapes=[
            pltpu.VMEM((BLOCKS, COMP, 32, 128), jnp.float32),
            pltpu.VMEM((BLOCKS, rows), jnp.int32),
            pltpu.VMEM((2, 32, 128), jnp.float32),
            pltpu.SMEM((1,), jnp.int32),
            pltpu.SMEM((1,), jnp.int32),
            pltpu.VMEM((slots, COMP, 8, 128), jnp.float32),
            pltpu.VMEM((slots, COMP, 8, 128), jnp.float32),
            pltpu.VMEM((slots, COMP, 8, 128), jnp.float32),
            pltpu.VMEM((2, 32, 128), jnp.float32),
            pltpu.VMEM((1, 128), jnp.float32),
            pltpu.VMEM((16, 1, 128), jnp.float32),
            pltpu.VMEM((32, 1, 128), jnp.float32),
            pltpu.SemaphoreType.DMA((6,)),
            pltpu.SemaphoreType.DMA((2,)),
            pltpu.SemaphoreType.DMA((slots,)),
            pltpu.SemaphoreType.DMA((slots,)),
            pltpu.SemaphoreType.DMA((slots,)),
            pltpu.SemaphoreType.DMA((slots,)),
            pltpu.SemaphoreType.DMA,
            pltpu.SemaphoreType.DMA,
            pltpu.SemaphoreType.DMA,
            pltpu.SemaphoreType.DMA,
            pltpu.SemaphoreType.REGULAR,
        ],
        compiler_params=pltpu.CompilerParams(collective_id=0, has_side_effects=True),
        name="smoother",
    )(packed_rows(block_values), block_cols, packed_rows(coarse_rhs), packed_rows(guess), bound_low, bound_high)
    return unpacked_rows(smoothed), unpacked_rows(residual), rms


def solution(mesh):
    finer = Mesh(mesh.devices.reshape(SIZES), AXES)
    return jax.shard_map(
        shards,
        mesh=finer,
        in_specs=(
            P(None, None, None, AXES),
            P(None, AXES),
            P(None, AXES),
            P(None, AXES),
            P(),
            P(),
        ),
        out_specs=(P(None, AXES), P(None, AXES), P()),
        check_vma=False,
    )
```
